256 devices in a mesh: grp: 2 (over z), tm: 128 (over x, y, core).
Axes of the slice: x: 8, y: 8, z: 2, core: 2. Of those that a mesh axis runs over, the one named last changes fastest.
The devices are a block of a 8x8x16 slice.
Arguments:
- samples: bfloat16 [16, 16777216], P('grp', 'tm'), parts along dimension 0, may hold values from -128 to 127, as said below
- filter_taps: bfloat16 [16, 8192], replicated, may hold values from -4 to 4
Outputs:
- channelized: bfloat16 [16, 2, 4096, 2048], P('grp', None, 'tm'), parts along dimension 0
The draws below stay inside these ranges and needn't reach their ends.
There are 2 independent parts, one for each index of `grp`. The reference program is written for one: setup_inputs(seed, part) draws one part's arguments, and reference() takes and returns one part's arrays. A program takes and returns all parts, laid end to end along the dimension named above; an argument that names none is the same for every part. Nothing has to cross between parts.
Inputs may be any that keep to these rules, and one draw needn't show every extreme that they name: `samples`: every sample is a whole number, as from an 8-bit converter.
All inputs are finite; a program needn't handle non-finite values.
Results may differ from the reference program's by a relative error of at most 0.007.
Values may be sent and summed in bfloat16 or wider, within the bound.
A program may use at most 128 MiB of HBM per device.

```python
import jax
import jax.numpy as jnp
from jax import lax

CHANNELS = 4096
FFT_LEN = 8192
ROW_LEN = 128
TAPS = 16
STREAMS = 8
SAMPLES = 16777216


def draw_samples(key, part):
    first_key, second_key = jax.random.split(jax.random.fold_in(key, 7))
    frame_total = SAMPLES // FFT_LEN
    base_level = jax.random.randint(first_key, (STREAMS, 1), 10, 61, dtype=jnp.int32)
    frame_index = (jnp.arange(SAMPLES, dtype=jnp.int32) // FFT_LEN)[None, :]
    amplitude = base_level * (frame_total + 2 * frame_index) // frame_total
    raw_bits = jax.random.randint(second_key, (STREAMS, SAMPLES), 0, 1048576, dtype=jnp.int32)
    values = raw_bits % (2 * amplitude + 1) - amplitude
    return jnp.clip(values, -128, 127).astype(jnp.bfloat16)


def scatter_about(key, extent, scale, bound, held_as=jnp.bfloat16):
    return jnp.clip(scale * jax.random.normal(key, extent, jnp.float32), -bound, bound).astype(held_as)


def setup_inputs(seed: int = 0, part: int = 0) -> dict:
    keys = jax.random.split(jax.random.key(seed), 3)
    part_keys = jax.random.split(jax.random.fold_in(keys[2], part), 3)
    samples = draw_samples(jax.random.fold_in(jax.random.fold_in(keys[2], part), 71), part)
    filter_taps = scatter_about(keys[1], (TAPS, FFT_LEN), 1.0, 4.0)
    return {"samples": samples, "filter_taps": filter_taps}


target_level = 0.378
epsilon = 1e-06

def tables(row_len, col_len):
    fft_len = row_len * col_len
    rows_a = jnp.arange(row_len, dtype=jnp.int32)
    cols_b = jnp.arange(col_len, dtype=jnp.int32)
    half_c = jnp.arange(col_len // 2, dtype=jnp.int32)
    angle_a = 2.0 * jnp.pi / row_len * (rows_a[:, None] * rows_a[None, :] % row_len).astype(jnp.float32)
    angle_t = 2.0 * jnp.pi / fft_len * (cols_b[:, None] * rows_a[None, :] % fft_len).astype(jnp.float32)
    angle_b = 2.0 * jnp.pi / col_len * (cols_b[:, None] * half_c[None, :] % col_len).astype(jnp.float32)
    return (jnp.cos(angle_a).astype(jnp.bfloat16), jnp.sin(angle_a).astype(jnp.bfloat16), jnp.cos(angle_t), jnp.sin(angle_t), jnp.cos(angle_b).astype(jnp.bfloat16), jnp.sin(angle_b).astype(jnp.bfloat16))

def transform(filtered):
    streams, frames, fft_len = filtered.shape
    col_len = fft_len // ROW_LEN
    cos_a, sin_a, cos_t, sin_t, cos_b, sin_b = tables(ROW_LEN, col_len)
    blocks = filtered.reshape(streams, frames, ROW_LEN, col_len).astype(jnp.float32)
    first_re = jnp.einsum('sfab,ad->sfbd', blocks, cos_a.astype(jnp.float32))
    first_im = -jnp.einsum('sfab,ad->sfbd', blocks, sin_a.astype(jnp.float32))
    twisted_re = lax.optimization_barrier((first_re * cos_t + first_im * sin_t).astype(jnp.bfloat16)).astype(jnp.float32)
    twisted_im = lax.optimization_barrier((first_im * cos_t - first_re * sin_t).astype(jnp.bfloat16)).astype(jnp.float32)
    cos_f = cos_b.astype(jnp.float32)
    sin_f = sin_b.astype(jnp.float32)
    spec_re = jnp.einsum('sfbd,bc->sfcd', twisted_re, cos_f) + jnp.einsum('sfbd,bc->sfcd', twisted_im, sin_f)
    spec_im = jnp.einsum('sfbd,bc->sfcd', twisted_im, cos_f) - jnp.einsum('sfbd,bc->sfcd', twisted_re, sin_f)
    return (spec_re.reshape(streams, frames, -1), spec_im.reshape(streams, frames, -1))

def reference(samples, filter_taps):
    streams = samples.shape[0]
    frames = samples.shape[1] // FFT_LEN
    signal = samples.astype(jnp.float32).reshape(streams, frames, FFT_LEN)
    extended = jnp.concatenate([jnp.zeros((streams, TAPS - 1, FFT_LEN), jnp.float32), signal], axis=1)
    weights = filter_taps.astype(jnp.float32)
    filtered = jnp.zeros((streams, frames, FFT_LEN), jnp.float32)
    for tap_index in range(TAPS):
        offset = TAPS - 1 - tap_index
        filtered = filtered + weights[tap_index] * extended[:, offset:offset + frames]
    filtered = filtered.astype(jnp.bfloat16)
    spec_re, spec_im = transform(filtered)
    spec_re = lax.optimization_barrier(spec_re.astype(jnp.bfloat16)).astype(jnp.float32)
    spec_im = lax.optimization_barrier(spec_im.astype(jnp.bfloat16)).astype(jnp.float32)
    power = lax.optimization_barrier(jnp.sum(spec_re * spec_re + spec_im * spec_im, axis=(1, 2)))
    gain = target_level / jnp.sqrt(power / (frames * CHANNELS) + epsilon)
    scaled = jnp.stack([spec_re, spec_im], axis=1) * gain[:, None, None, None]
    clipped = jnp.clip(scaled, -1.0, 1.0)
    return jnp.transpose(clipped, (0, 1, 3, 2)).astype(jnp.bfloat16)
```

```python
import functools
import math

import jax
import jax.numpy as jnp
import numpy as np
from jax import lax
from jax.experimental import pallas as pl
from jax.experimental.pallas import tpu as pltpu
from jax.sharding import PartitionSpec as P

MESH = pl.DeviceIdType.MESH
LANES = 128
PITCH = 136

target_level = 0.378
epsilon = 1e-06


def constants(streams, rows, half):
    t = np.arange(rows)
    lane = np.arange(LANES)
    k1 = np.arange(rows)
    k2 = np.arange(half)
    size = rows * LANES
    groups = streams // 4
    angle = 2.0 * np.pi * ((k1[:, None] * t[None, :]) % rows) / rows
    lower = rows // 2
    tables = [np.cos(angle)[:lower], np.sin(angle)[:lower]]
    tables[1][0] = np.cos(angle)[lower]
    first = np.zeros((2, groups, 4, lower, rows, streams), np.float32)
    for part, table in enumerate(tables):
        for s in range(streams):
            first[part, s // 4, s % 4, :, :, s] = table
    first = first.reshape(2 * groups * 4 * lower, rows * streams)
    upper = (rows - np.arange(lower)) % rows
    upper[0] = lower
    theta = np.stack([np.arange(lower), upper])
    theta = 2.0 * np.pi * ((theta[:, :, None] * lane) % size) / size
    twiddle = np.stack([np.cos(theta), np.sin(theta)]).astype(np.float32)
    turn = np.zeros((2, 4, lower, 4, lower), np.float32)
    for s in range(4):
        for k in range(lower):
            turn[0, s, k, s, k] = 1.0
            turn[1, s, k, s, (lower - k) % lower] = 1.0
    turn = turn.reshape(2, LANES, LANES)
    angle = 2.0 * np.pi * ((k2[:, None] * lane[None, :]) % LANES) / LANES
    cosine, sine = np.cos(angle), np.sin(angle)
    second = np.concatenate(
        [
            np.concatenate([cosine, -sine], axis=1),
            np.concatenate([-sine, -cosine], axis=1),
        ],
        axis=0,
    )
    return first, twiddle, second, turn


def kernel(
    dims,
    x_ref,
    taps_ref,
    first_ref,
    tw_ref,
    second_ref,
    recv,
    gain_ref,
    ext,
    taps_in,
    taps_wide,
    first,
    tw,
    second,
    filt,
    mixed,
    spread,
    send,
    acc,
    power_out,
    power_in,
    power_mid,
    power_cols,
    load_sem,
    halo_send_next,
    halo_send_prev,
    halo_prev,
    halo_next,
    data_send,
    data_recv,
    power_send,
    power_recv,
    power_send_mid,
    power_recv_mid,
    first_sem,
    edge_sem,
    chain_sem,
    ends_sem,
    all_sem,
):
    n, side, frames, taps, fft_len, streams, rows, half = dims
    me = lax.axis_index("tm")
    mx, my, mc = me // (2 * side), lax.rem(me // 2, side), lax.rem(me, 2)
    nxt, prv = lax.rem(me + 1, n), lax.rem(me + n - 1, n)
    width = 2 * side
    block = frames // 2
    back = taps - 1 - block

    def signal(sem, to):
        pl.semaphore_signal(sem, inc=1, device_id={"tm": to}, device_id_type=MESH)

    place = lax.rem(me, width)
    starts, ends = place == 0, place == width - 1
    barrier = pltpu.get_barrier_semaphore()

    @pl.when((me != 0) & (place < width - 1))
    def _():
        signal(barrier, nxt)

    @pl.when(me != 0)
    def _():
        signal(barrier, prv)

    @pl.when(ends)
    def _():
        for i in range(1, side):
            signal(barrier, lax.rem(me + width * i, n))

    @pl.when(me == n - 1)
    def _():
        signal(barrier, 0)

    loads = [
        pltpu.make_async_copy(taps_ref, taps_in, load_sem.at[0]),
        pltpu.make_async_copy(first_ref, first, load_sem.at[1]),
        pltpu.make_async_copy(tw_ref, tw, load_sem.at[2]),
        pltpu.make_async_copy(second_ref, second, load_sem.at[3]),
    ]
    for copy in loads:
        copy.start()
    own = []
    for f in range(frames):
        copy = pltpu.make_async_copy(
            x_ref.at[:, pl.ds(f * fft_len, fft_len)], ext.at[back + f], load_sem.at[5 + f]
        )
        copy.start()
        own.append(copy)

    expected = jnp.where(ends, side + 1, jnp.where(starts, 1, 2))
    expected = expected + jnp.where(me == 0, 1, 0)
    expected = expected - jnp.where((me == 1) | (me == n - 1), 1, 0)
    pl.semaphore_wait(barrier, expected)

    def to_next():
        for i in range(back - 1, -1, -1):
            pltpu.make_async_remote_copy(
                src_ref=x_ref.at[:, pl.ds((frames - back + i) * fft_len, fft_len)],
                dst_ref=ext.at[i],
                send_sem=halo_send_next,
                recv_sem=halo_prev,
                device_id={"tm": nxt},
                device_id_type=MESH,
            ).start()

    def to_previous():
        for i in range(block):
            pltpu.make_async_remote_copy(
                src_ref=x_ref.at[:, pl.ds(i * fft_len, fft_len)],
                dst_ref=ext.at[back + frames + i],
                send_sem=halo_send_prev,
                recv_sem=halo_next,
                device_id={"tm": prv},
                device_id_type=MESH,
            ).start()

    pl.when(me != n - 1)(to_next)
    pl.when((me == 0) | (place > 1) | ((place == 1) & (me != 1)))(to_previous)

    @pl.when(me == 0)
    def _():
        signal(first_sem, 1)
        signal(first_sem, n - 1)

    @pl.when(ends & (me != n - 1))
    def _():
        signal(edge_sem, nxt)

    @pl.when((place > 0) & (me != 1))
    def _():
        pl.semaphore_wait(chain_sem, 1)

    @pl.when((me != 0) & (place < width - 1))
    def _():
        signal(chain_sem, nxt)

    loads[0].wait()

    def widen(t, carry):
        lanes = pl.ds(pl.multiple_of(t * LANES, LANES), LANES)
        part = taps_in[:, lanes].astype(jnp.float32)
        for p in range(taps):
            taps_wide[t, p] = jnp.broadcast_to(part[p : p + 1, :], (streams, LANES))
        return carry

    lax.fori_loop(0, rows, widen, 0)

    for copy in loads[1:] + own:
        copy.wait()
    acc[...] = jnp.zeros_like(acc)

    def blanked(start, count):
        def blank(i, carry):
            ext[start + i] = jnp.zeros((streams, fft_len), jnp.bfloat16)
            return carry

        lax.fori_loop(0, count, blank, 0)

    def which_of(step):
        return lax.rem(1 + step + mc + jnp.where(me < 2, 1, 0), 2)

    def slot_of(which):
        into = lax.rem(2 * me + 1 + which, 2 * n)
        return pl.ds(pl.multiple_of(into * block, block), block)

    def send_data(step, which, to):
        pltpu.make_async_remote_copy(
            src_ref=send.at[step, to],
            dst_ref=recv.at[:, slot_of(which), :],
            send_sem=data_send,
            recv_sem=data_recv,
            device_id={"tm": to},
            device_id_type=MESH,
        ).start()

    def group(step, carry):
        which = which_of(step)
        base = which * block

        @pl.when((which == 0) & (me != 0))
        def _():
            ahead = ext.at[pl.ds(0, back)]
            pltpu.make_async_copy(ahead, ahead, halo_prev).wait()

        @pl.when((which == 0) & (me == 0))
        def _():
            blanked(0, back)

        @pl.when(which == 1)
        def _():
            behind = ext.at[pl.ds(back + frames, block)]
            pltpu.make_async_copy(behind, behind, halo_next).wait()

        @pl.when((which == 1) & (me == n - 1))
        def _():
            blanked(block, back + frames - block)

        def filtering(pair, carry):
            pieces = []
            for u in range(2):
                t = 2 * pair + u
                lanes = pl.ds(pl.multiple_of(t * LANES, LANES), LANES)
                window = [
                    ext[base + i, :, lanes].astype(jnp.float32) for i in range(taps - 1 + block)
                ]
                sums = [None] * block
                for p in range(taps):
                    weight = taps_wide[t, p]
                    for o in range(block):
                        term = weight * window[taps - 1 + o - p]
                        sums[o] = term if sums[o] is None else sums[o] + term
                pieces.append(sums)
            to = pl.ds(pl.multiple_of(pair * 2 * streams, 2 * streams), 2 * streams)
            for o in range(block):
                filt[o, to, :] = jnp.concatenate([pieces[0][o], pieces[1][o]], axis=0).astype(
                    jnp.bfloat16
                )
            return carry

        lax.fori_loop(0, rows // 2, filtering, 0)

        @pl.when((step == 0) & ends)
        def _():
            for i in range(1, side):
                signal(ends_sem, lax.rem(me + width * i, n))

        part_rows = first.shape[0] // 2
        lower = rows // 2
        tables = [[tw[part, h][None] for h in range(2)] for part in range(2)]
        top = lax.broadcasted_iota(jnp.int32, (4, 8, LANES), 1) == 0

        def first_stage(pair):
            both = jnp.concatenate([filt[2 * pair], filt[2 * pair + 1]], axis=1)
            mixed[pair % 2] = jnp.dot(first[...], both, preferred_element_type=jnp.float32)

        first_stage(0)
        for pair in range(block // 2):
            if pair + 1 < block // 2:
                first_stage(pair + 1)
            for u in range(2):
                at = pl.ds((2 * pair + u) * PITCH, 2 * half)
                lanes = slice(u * LANES, (u + 1) * LANES)
                for q in range(streams // 4):
                    rows_q = slice(q * 4 * lower, (q + 1) * 4 * lower)
                    rows_s = slice(part_rows + q * 4 * lower, part_rows + (q + 1) * 4 * lower)
                    even = mixed[pair % 2, rows_q, lanes].reshape(4, lower, LANES)
                    odd = mixed[pair % 2, rows_s, lanes].reshape(4, lower, LANES)
                    im = jnp.concatenate([jnp.where(top, 0.0, odd[:, :8]), odd[:, 8:]], axis=1)
                    re = jnp.concatenate(
                        [jnp.where(top, odd[:, :8], even[:, :8]), even[:, 8:]], axis=1
                    )
                    (cos_0, cos_1), (sin_0, sin_1) = tables
                    real = jnp.concatenate(
                        [even * cos_0 - im * sin_0, re * cos_1 + im * sin_1], axis=0
                    )
                    imag = jnp.concatenate(
                        [even * sin_0 + im * cos_0, re * sin_1 - im * cos_1], axis=0
                    )
                    twisted = jnp.concatenate(
                        [
                            real.reshape(8 * lower, LANES).astype(jnp.bfloat16),
                            imag.reshape(8 * lower, LANES).astype(jnp.bfloat16),
                        ],
                        axis=1,
                    )
                    spec = lax.dot_general(
                        second[...],
                        twisted,
                        (((1,), (1,)), ((), ())),
                        preferred_element_type=jnp.float32,
                    )
                    spread[2 * q, at, :] = spec[:, :LANES]
                    spread[2 * q + 1, at, :] = spec[:, LANES:]

        def packing(k, carry):
            sums = list(carry)
            for h in range(2):
                for q in range(streams // 4):
                    for part in range(2):
                        piece = spread.at[2 * q + h][pl.ds(part * half + k, block, stride=PITCH), :]
                        piece = piece.astype(jnp.bfloat16)
                        send[step, 2 * k + h, 2 * q + part] = piece
                        wide = piece.astype(jnp.float32)
                        sums[q] = sums[q] + wide * wide
            return tuple(sums)

        sums = lax.fori_loop(
            0, half, packing, tuple(acc[q] for q in range(streams // 4)), unroll=2
        )
        for q in range(streams // 4):
            acc[q] = sums[q]

        @pl.when((step == 0) & starts & (me != 0))
        def _():
            pl.semaphore_wait(edge_sem, 1)
            to_previous()

        @pl.when((step == 0) & (me == 1))
        def _():
            pl.semaphore_wait(first_sem, 1)
            to_previous()

        @pl.when((step == 0) & ends)
        def _():
            pl.semaphore_wait(ends_sem, side - 1)
            for i in range(1, width):
                to = me - i

                @pl.when(to != 0)
                def _():
                    signal(all_sem, to)

        @pl.when((step == 0) & jnp.logical_not(ends))
        def _():
            pl.semaphore_wait(all_sem, 1)

        @pl.when((step == 0) & (me == 1))
        def _():
            signal(all_sem, 0)

        @pl.when((step == 0) & (me == 0))
        def _():
            def here(i, carry):
                signal(first_sem, i)
                return carry

            lax.fori_loop(2, n - 1, here, 0, unroll=4)

        @pl.when((step == 1) & (me > 1))
        def _():
            pl.semaphore_wait(first_sem, 1)

        @pl.when(step == 1)
        def _():
            lane = lax.broadcasted_iota(jnp.int32, (block, LANES), 1)
            low = acc[0] + pltpu.roll(acc[0], LANES - 16, 1)
            high = acc[1] + pltpu.roll(acc[1], LANES - 16, 1)
            row = jnp.where(lane % 32 < 16, low, pltpu.roll(high, 16, 1))
            row = jnp.sum(row, axis=0, keepdims=True)
            power_out[...] = row
            power_in[place] = row
            for i in range(1, width):
                to = lax.rem(place + i, width)
                pltpu.make_async_remote_copy(
                    src_ref=power_out,
                    dst_ref=power_in.at[place],
                    send_sem=power_send,
                    recv_sem=power_recv,
                    device_id={"tm": mx * width + to},
                    device_id_type=MESH,
                ).start()

        def sending(d, carry):
            pair = d // 2
            dy = lax.rem(pair, side)
            dx = lax.rem(pair // side + 3 * dy, side)
            to = (
                lax.rem(mx + dx, side) * width
                + lax.rem(my + dy, side) * 2
                + lax.rem(mc + lax.rem(d, 2), 2)
            )

            @pl.when((to != 0) | (step == 1) | (me == 0))
            def _():
                send_data(step, which, to)

            @pl.when((to == 0) & (step == 1))
            def _():
                send_data(0, which_of(0), to)

            return carry

        lax.fori_loop(1, n, sending, 0, unroll=4)
        return carry

    lax.fori_loop(0, 2, group, 0)

    kept = []
    for step in range(2):
        copy = pltpu.make_async_copy(
            send.at[step, me], recv.at[:, slot_of(which_of(step)), :], load_sem.at[3 + step]
        )
        copy.start()
        kept.append(copy)

    others = power_in.at[pl.ds(0, width - 1)]
    pltpu.make_async_copy(others, others, power_recv).wait()
    row = jnp.sum(power_in[...], axis=0)
    power_mid[...] = row
    power_cols[mx] = row
    for i in range(1, side):
        pltpu.make_async_remote_copy(
            src_ref=power_mid,
            dst_ref=power_cols.at[mx],
            send_sem=power_send_mid,
            recv_sem=power_recv_mid,
            device_id={"tm": lax.rem(me + width * i, n)},
            device_id_type=MESH,
        ).start()
    columns = power_cols.at[pl.ds(0, side - 1)]
    pltpu.make_async_copy(columns, columns, power_recv_mid).wait()
    total = jnp.sum(power_cols[...], axis=0)
    lane = lax.broadcasted_iota(jnp.int32, (1, LANES), 1)
    count = frames * n * half * rows
    gains = []
    for s in range(streams):
        start = (s % 4) * 32 + (s // 4) * 16
        power = jnp.sum(
            jnp.where((lane >= start) & (lane < start + 16), total, 0.0), axis=1, keepdims=True
        )
        gains.append(target_level / jnp.sqrt(power / count + epsilon))

    level = jnp.zeros((streams, LANES), jnp.float32)
    index = lax.broadcasted_iota(jnp.int32, (streams, LANES), 0)
    for s in range(streams):
        level = jnp.where(index == s, gains[s], level)
    gain_ref[...] = level

    arrived = recv.at[:, pl.ds(0, (n - 1) * frames), :]
    pltpu.make_async_copy(arrived, arrived, data_recv).wait()
    for copy in kept:
        copy.wait()

    @pl.when(me != n - 1)
    def _():
        sent = ext.at[pl.ds(0, back)]
        pltpu.make_async_copy(sent, sent, halo_send_next).wait()

    sent = ext.at[pl.ds(0, block)]
    pltpu.make_async_copy(sent, sent, halo_send_prev).wait()
    pltpu.make_async_copy(arrived, arrived, data_send).wait()
    pltpu.make_async_copy(others, others, power_send).wait()
    pltpu.make_async_copy(columns, columns, power_send_mid).wait()


def finish(rows, turn_ref, gain_ref, spectra_ref, out_ref):
    for q in range(spectra_ref.shape[0] // 2):
        for part in range(2):
            turned = lax.dot_general(
                turn_ref[...],
                spectra_ref[2 * q + part],
                (((1,), (1,)), ((), ())),
                preferred_element_type=jnp.float32,
            )
            for s in range(4):
                gain = gain_ref[4 * q + s : 4 * q + s + 1, :1]
                scaled = turned[s * rows : (s + 1) * rows, :] * gain
                out_ref[4 * q + s, part] = jnp.clip(scaled, -1.0, 1.0).astype(jnp.bfloat16)


def solution(mesh):
    n = mesh.shape["tm"]
    side = math.isqrt(n // 2)

    def on_device(samples, filter_taps):
        streams, length = samples.shape
        taps, fft_len = filter_taps.shape
        frames = length // fft_len
        rows = fft_len // LANES
        half = rows
        block = frames // 2
        back = taps - 1 - block
        first, twiddle, second, turn = constants(streams, rows, half)
        first = jnp.asarray(first, jnp.bfloat16)
        second = jnp.asarray(second, jnp.bfloat16)
        eye = jnp.asarray(turn, jnp.bfloat16)
        dims = (n, side, frames, taps, fft_len, streams, rows, half)
        tiles = streams // 4
        per = fft_len // 2 // n

        def body(*refs):
            kernel(dims, *refs)

        anywhere = pl.BlockSpec(memory_space=pltpu.HBM)
        dma = pltpu.SemaphoreType.DMA
        spectra, gain = pl.pallas_call(
            body,
            out_shape=(
                jax.ShapeDtypeStruct((2 * tiles, n * frames, LANES), jnp.bfloat16),
                jax.ShapeDtypeStruct((streams, LANES), jnp.float32),
            ),
            in_specs=[anywhere] * 5,
            out_specs=(anywhere, pl.BlockSpec(memory_space=pltpu.VMEM)),
            scratch_shapes=[
                pltpu.VMEM((back + frames + block, streams, fft_len), jnp.bfloat16),
                pltpu.VMEM((taps, fft_len), jnp.bfloat16),
                pltpu.VMEM((rows, taps, streams, LANES), jnp.float32),
                pltpu.VMEM(first.shape, jnp.bfloat16),
                pltpu.VMEM(twiddle.shape, jnp.float32),
                pltpu.VMEM(second.shape, jnp.bfloat16),
                pltpu.VMEM((block, rows * streams, LANES), jnp.bfloat16),
                pltpu.VMEM((2, first.shape[0], 2 * LANES), jnp.float32),
                pltpu.VMEM((2 * tiles, block * PITCH, LANES), jnp.float32),
                pltpu.VMEM((2, n, 2 * tiles, block, LANES), jnp.bfloat16),
                pltpu.VMEM((tiles, block, LANES), jnp.float32),
                pltpu.VMEM((1, LANES), jnp.float32),
                pltpu.VMEM((2 * side, 1, LANES), jnp.float32),
                pltpu.VMEM((1, LANES), jnp.float32),
                pltpu.VMEM((side, 1, LANES), jnp.float32),
                dma((5 + frames,)),
                dma,
                dma,
                dma,
                dma,
                dma,
                dma,
                dma,
                dma,
                dma,
                dma,
                pltpu.SemaphoreType.REGULAR,
                pltpu.SemaphoreType.REGULAR,
                pltpu.SemaphoreType.REGULAR,
                pltpu.SemaphoreType.REGULAR,
                pltpu.SemaphoreType.REGULAR,
            ],
            compiler_params=pltpu.CompilerParams(
                collective_id=1, has_side_effects=True, vmem_limit_bytes=63 * 1024 * 1024
            ),
        )(samples, filter_taps, first, jnp.asarray(twiddle), second)

        cols = 1024

        def by_half(i):
            return (lax.rem(lax.axis_index("tm"), 2), 0, 0)

        return pl.pallas_call(
            functools.partial(finish, rows // 2),
            grid=(frames * n // cols,),
            out_shape=jax.ShapeDtypeStruct((streams, 2, per, frames * n), jnp.bfloat16),
            in_specs=[
                pl.BlockSpec((None, LANES, LANES), by_half),
                pl.BlockSpec((streams, LANES), lambda i: (0, 0)),
                pl.BlockSpec((2 * tiles, cols, LANES), lambda i: (0, i, 0)),
            ],
            out_specs=pl.BlockSpec((streams, 2, per, cols), lambda i: (0, 0, 0, i)),
        )(eye, gain, spectra)

    return jax.shard_map(
        on_device,
        mesh=mesh,
        in_specs=(P("grp", "tm"), P()),
        out_specs=P("grp", None, "tm", None),
        check_vma=False,
    )
```

```python
import functools
import math

import jax
import jax.numpy as jnp
import numpy as np
from jax import lax
from jax.experimental import pallas as pl
from jax.experimental.pallas import tpu as pltpu
from jax.sharding import PartitionSpec as P

MESH = pl.DeviceIdType.MESH
LANES = 128
PITCH = 136

target_level = 0.378
epsilon = 1e-06


def constants(streams, rows, half):
    t = np.arange(rows)
    lane = np.arange(LANES)
    k1 = np.arange(rows)
    k2 = np.arange(half)
    size = rows * LANES
    groups = streams // 4
    angle = 2.0 * np.pi * ((k1[:, None] * t[None, :]) % rows) / rows
    lower = rows // 2
    tables = [np.cos(angle)[:lower], np.sin(angle)[:lower]]
    tables[1][0] = np.cos(angle)[lower]
    first = np.zeros((2, groups, 4, lower, rows, streams), np.float32)
    for part, table in enumerate(tables):
        for s in range(streams):
            first[part, s // 4, s % 4, :, :, s] = table
    first = first.reshape(2 * groups * 4 * lower, rows * streams)
    upper = (rows - np.arange(lower)) % rows
    upper[0] = lower
    theta = np.stack([np.arange(lower), upper])
    theta = 2.0 * np.pi * ((theta[:, :, None] * lane) % size) / size
    twiddle = np.stack([np.cos(theta), np.sin(theta)]).astype(np.float32)
    turn = np.zeros((2, 4, lower, 4, lower), np.float32)
    for s in range(4):
        for k in range(lower):
            turn[0, s, k, s, k] = 1.0
            turn[1, s, k, s, (lower - k) % lower] = 1.0
    turn = turn.reshape(2, LANES, LANES)
    angle = 2.0 * np.pi * ((k2[:, None] * lane[None, :]) % LANES) / LANES
    cosine, sine = np.cos(angle), np.sin(angle)
    second = np.concatenate(
        [
            np.concatenate([cosine, -sine], axis=1),
            np.concatenate([-sine, -cosine], axis=1),
        ],
        axis=0,
    )
    return first, twiddle, second, turn


def kernel(
    dims,
    x_ref,
    taps_ref,
    first_ref,
    tw_ref,
    second_ref,
    recv,
    gain_ref,
    ext,
    taps_in,
    taps_wide,
    first,
    tw,
    second,
    filt,
    mixed,
    spread,
    send,
    acc,
    power_out,
    power_in,
    power_mid,
    power_cols,
    load_sem,
    halo_send_next,
    halo_send_prev,
    halo_prev,
    halo_next,
    data_send,
    data_recv,
    power_send,
    power_recv,
    power_send_mid,
    power_recv_mid,
    first_sem,
    edge_sem,
    chain_sem,
    ends_sem,
    all_sem,
):
    n, side, frames, taps, fft_len, streams, rows, half = dims
    me = lax.axis_index("tm")
    mx, my, mc = me // (2 * side), lax.rem(me // 2, side), lax.rem(me, 2)
    nxt, prv = lax.rem(me + 1, n), lax.rem(me + n - 1, n)
    width = 2 * side
    block = frames // 2
    back = taps - 1 - block

    def signal(sem, to):
        pl.semaphore_signal(sem, inc=1, device_id={"tm": to}, device_id_type=MESH)

    place = lax.rem(me, width)
    starts, ends = place == 0, place == width - 1
    barrier = pltpu.get_barrier_semaphore()

    @pl.when((me != 0) & (place < width - 1))
    def _():
        signal(barrier, nxt)

    @pl.when(me != 0)
    def _():
        signal(barrier, prv)

    @pl.when(ends)
    def _():
        for i in range(1, side):
            signal(barrier, lax.rem(me + width * i, n))

    @pl.when(me == n - 1)
    def _():
        signal(barrier, 0)

    loads = [
        pltpu.make_async_copy(taps_ref, taps_in, load_sem.at[0]),
        pltpu.make_async_copy(first_ref, first, load_sem.at[1]),
        pltpu.make_async_copy(tw_ref, tw, load_sem.at[2]),
        pltpu.make_async_copy(second_ref, second, load_sem.at[3]),
    ]
    for copy in loads:
        copy.start()
    own = []
    for f in range(frames):
        copy = pltpu.make_async_copy(
            x_ref.at[:, pl.ds(f * fft_len, fft_len)], ext.at[back + f], load_sem.at[5 + f]
        )
        copy.start()
        own.append(copy)

    expected = jnp.where(ends, side + 1, jnp.where(starts, 1, 2))
    expected = expected + jnp.where(me == 0, 1, 0)
    expected = expected - jnp.where((me == 1) | (me == n - 1), 1, 0)
    pl.semaphore_wait(barrier, expected)

    def to_next():
        for i in range(back - 1, -1, -1):
            pltpu.make_async_remote_copy(
                src_ref=x_ref.at[:, pl.ds((frames - back + i) * fft_len, fft_len)],
                dst_ref=ext.at[i],
                send_sem=halo_send_next,
                recv_sem=halo_prev,
                device_id={"tm": nxt},
                device_id_type=MESH,
            ).start()

    def to_previous():
        for i in range(block):
            pltpu.make_async_remote_copy(
                src_ref=x_ref.at[:, pl.ds(i * fft_len, fft_len)],
                dst_ref=ext.at[back + frames + i],
                send_sem=halo_send_prev,
                recv_sem=halo_next,
                device_id={"tm": prv},
                device_id_type=MESH,
            ).start()

    pl.when(me != n - 1)(to_next)
    pl.when((me == 0) | (place > 1) | ((place == 1) & (me != 1)))(to_previous)

    @pl.when(me == 0)
    def _():
        signal(first_sem, 1)
        signal(first_sem, n - 1)

    @pl.when(ends & (me != n - 1))
    def _():
        signal(edge_sem, nxt)

    @pl.when((place > 0) & (me != 1))
    def _():
        pl.semaphore_wait(chain_sem, 1)

    @pl.when((me != 0) & (place < width - 1))
    def _():
        signal(chain_sem, nxt)

    loads[0].wait()

    def widen(t, carry):
        lanes = pl.ds(pl.multiple_of(t * LANES, LANES), LANES)
        part = taps_in[:, lanes].astype(jnp.float32)
        for p in range(taps):
            taps_wide[t, p] = jnp.broadcast_to(part[p : p + 1, :], (streams, LANES))
        return carry

    lax.fori_loop(0, rows, widen, 0)

    for copy in loads[1:] + own:
        copy.wait()
    acc[...] = jnp.zeros_like(acc)

    def blanked(start, count):
        def blank(i, carry):
            ext[start + i] = jnp.zeros((streams, fft_len), jnp.bfloat16)
            return carry

        lax.fori_loop(0, count, blank, 0)

    def which_of(step):
        return lax.rem(1 + step + mc + jnp.where(me < 2, 1, 0), 2)

    def slot_of(which):
        into = lax.rem(2 * me + 1 + which, 2 * n)
        return into

    def send_data(step, which, to):
        pltpu.make_async_remote_copy(
            src_ref=send.at[step, to],
            dst_ref=recv.at[slot_of(which)],
            send_sem=data_send,
            recv_sem=data_recv,
            device_id={"tm": to},
            device_id_type=MESH,
        ).start()

    def group(step, carry):
        which = which_of(step)
        base = which * block

        @pl.when((which == 0) & (me != 0))
        def _():
            ahead = ext.at[pl.ds(0, back)]
            pltpu.make_async_copy(ahead, ahead, halo_prev).wait()

        @pl.when((which == 0) & (me == 0))
        def _():
            blanked(0, back)

        @pl.when(which == 1)
        def _():
            behind = ext.at[pl.ds(back + frames, block)]
            pltpu.make_async_copy(behind, behind, halo_next).wait()

        @pl.when((which == 1) & (me == n - 1))
        def _():
            blanked(block, back + frames - block)

        def filtering(pair, carry):
            pieces = []
            for u in range(2):
                t = 2 * pair + u
                lanes = pl.ds(pl.multiple_of(t * LANES, LANES), LANES)
                window = [
                    ext[base + i, :, lanes].astype(jnp.float32) for i in range(taps - 1 + block)
                ]
                sums = [None] * block
                for p in range(taps):
                    weight = taps_wide[t, p]
                    for o in range(block):
                        term = weight * window[taps - 1 + o - p]
                        sums[o] = term if sums[o] is None else sums[o] + term
                pieces.append(sums)
            to = pl.ds(pl.multiple_of(pair * 2 * streams, 2 * streams), 2 * streams)
            for o in range(block):
                filt[o, to, :] = jnp.concatenate([pieces[0][o], pieces[1][o]], axis=0).astype(
                    jnp.bfloat16
                )
            return carry

        lax.fori_loop(0, rows // 2, filtering, 0)

        @pl.when((step == 0) & ends)
        def _():
            for i in range(1, side):
                signal(ends_sem, lax.rem(me + width * i, n))

        part_rows = first.shape[0] // 2
        lower = rows // 2
        tables = [[tw[part, h][None] for h in range(2)] for part in range(2)]
        top = lax.broadcasted_iota(jnp.int32, (4, 8, LANES), 1) == 0

        def first_stage(pair):
            both = jnp.concatenate([filt[2 * pair], filt[2 * pair + 1]], axis=1)
            mixed[pair % 2] = jnp.dot(first[...], both, preferred_element_type=jnp.float32)

        first_stage(0)
        for pair in range(block // 2):
            if pair + 1 < block // 2:
                first_stage(pair + 1)
            for u in range(2):
                at = pl.ds((2 * pair + u) * PITCH, 2 * half)
                lanes = slice(u * LANES, (u + 1) * LANES)
                for q in range(streams // 4):
                    rows_q = slice(q * 4 * lower, (q + 1) * 4 * lower)
                    rows_s = slice(part_rows + q * 4 * lower, part_rows + (q + 1) * 4 * lower)
                    even = mixed[pair % 2, rows_q, lanes].reshape(4, lower, LANES)
                    odd = mixed[pair % 2, rows_s, lanes].reshape(4, lower, LANES)
                    im = jnp.concatenate([jnp.where(top, 0.0, odd[:, :8]), odd[:, 8:]], axis=1)
                    re = jnp.concatenate(
                        [jnp.where(top, odd[:, :8], even[:, :8]), even[:, 8:]], axis=1
                    )
                    (cos_0, cos_1), (sin_0, sin_1) = tables
                    real = jnp.concatenate(
                        [even * cos_0 - im * sin_0, re * cos_1 + im * sin_1], axis=0
                    )
                    imag = jnp.concatenate(
                        [even * sin_0 + im * cos_0, re * sin_1 - im * cos_1], axis=0
                    )
                    twisted = jnp.concatenate(
                        [
                            real.reshape(8 * lower, LANES).astype(jnp.bfloat16),
                            imag.reshape(8 * lower, LANES).astype(jnp.bfloat16),
                        ],
                        axis=1,
                    )
                    spec = lax.dot_general(
                        second[...],
                        twisted,
                        (((1,), (1,)), ((), ())),
                        preferred_element_type=jnp.float32,
                    )
                    spread[2 * q, at, :] = spec[:, :LANES]
                    spread[2 * q + 1, at, :] = spec[:, LANES:]

        def packing(k, carry):
            sums = list(carry)
            for h in range(2):
                for q in range(streams // 4):
                    for part in range(2):
                        piece = spread.at[2 * q + h][pl.ds(part * half + k, block, stride=PITCH), :]
                        piece = piece.astype(jnp.bfloat16)
                        send[step, 2 * k + h, 2 * q + part] = piece
                        wide = piece.astype(jnp.float32)
                        sums[q] = sums[q] + wide * wide
            return tuple(sums)

        sums = lax.fori_loop(
            0, half, packing, tuple(acc[q] for q in range(streams // 4)), unroll=2
        )
        for q in range(streams // 4):
            acc[q] = sums[q]

        @pl.when((step == 0) & starts & (me != 0))
        def _():
            pl.semaphore_wait(edge_sem, 1)
            to_previous()

        @pl.when((step == 0) & (me == 1))
        def _():
            pl.semaphore_wait(first_sem, 1)
            to_previous()

        @pl.when((step == 0) & ends)
        def _():
            pl.semaphore_wait(ends_sem, side - 1)
            for i in range(1, width):
                to = me - i

                @pl.when(to != 0)
                def _():
                    signal(all_sem, to)

        @pl.when((step == 0) & jnp.logical_not(ends))
        def _():
            pl.semaphore_wait(all_sem, 1)

        @pl.when((step == 0) & (me == 1))
        def _():
            signal(all_sem, 0)

        @pl.when((step == 0) & (me == 0))
        def _():
            def here(i, carry):
                signal(first_sem, i)
                return carry

            lax.fori_loop(2, n - 1, here, 0, unroll=4)

        @pl.when((step == 1) & (me > 1))
        def _():
            pl.semaphore_wait(first_sem, 1)

        @pl.when(step == 1)
        def _():
            lane = lax.broadcasted_iota(jnp.int32, (block, LANES), 1)
            low = acc[0] + pltpu.roll(acc[0], LANES - 16, 1)
            high = acc[1] + pltpu.roll(acc[1], LANES - 16, 1)
            row = jnp.where(lane % 32 < 16, low, pltpu.roll(high, 16, 1))
            row = jnp.sum(row, axis=0, keepdims=True)
            power_out[...] = row
            power_in[place] = row
            for i in range(1, width):
                to = lax.rem(place + i, width)
                pltpu.make_async_remote_copy(
                    src_ref=power_out,
                    dst_ref=power_in.at[place],
                    send_sem=power_send,
                    recv_sem=power_recv,
                    device_id={"tm": mx * width + to},
                    device_id_type=MESH,
                ).start()

        def sending(d, carry):
            pair = d // 2
            dy = lax.rem(pair, side)
            dx = lax.rem(pair // side + 3 * dy, side)
            to = (
                lax.rem(mx + dx, side) * width
                + lax.rem(my + dy, side) * 2
                + lax.rem(mc + lax.rem(d, 2), 2)
            )

            @pl.when((to != 0) | (step == 1) | (me == 0))
            def _():
                send_data(step, which, to)

            @pl.when((to == 0) & (step == 1))
            def _():
                send_data(0, which_of(0), to)

            return carry

        lax.fori_loop(1, n, sending, 0, unroll=4)
        return carry

    lax.fori_loop(0, 2, group, 0)

    kept = []
    for step in range(2):
        copy = pltpu.make_async_copy(
            send.at[step, me], recv.at[slot_of(which_of(step))], load_sem.at[3 + step]
        )
        copy.start()
        kept.append(copy)

    others = power_in.at[pl.ds(0, width - 1)]
    pltpu.make_async_copy(others, others, power_recv).wait()
    row = jnp.sum(power_in[...], axis=0)
    power_mid[...] = row
    power_cols[mx] = row
    for i in range(1, side):
        pltpu.make_async_remote_copy(
            src_ref=power_mid,
            dst_ref=power_cols.at[mx],
            send_sem=power_send_mid,
            recv_sem=power_recv_mid,
            device_id={"tm": lax.rem(me + width * i, n)},
            device_id_type=MESH,
        ).start()
    columns = power_cols.at[pl.ds(0, side - 1)]
    pltpu.make_async_copy(columns, columns, power_recv_mid).wait()
    total = jnp.sum(power_cols[...], axis=0)
    lane = lax.broadcasted_iota(jnp.int32, (1, LANES), 1)
    count = frames * n * half * rows
    gains = []
    for s in range(streams):
        start = (s % 4) * 32 + (s // 4) * 16
        power = jnp.sum(
            jnp.where((lane >= start) & (lane < start + 16), total, 0.0), axis=1, keepdims=True
        )
        gains.append(target_level / jnp.sqrt(power / count + epsilon))

    level = jnp.zeros((streams, LANES), jnp.float32)
    index = lax.broadcasted_iota(jnp.int32, (streams, LANES), 0)
    for s in range(streams):
        level = jnp.where(index == s, gains[s], level)
    gain_ref[...] = level

    arrived = recv.at[pl.ds(0, 2 * (n - 1))]
    pltpu.make_async_copy(arrived, arrived, data_recv).wait()
    for copy in kept:
        copy.wait()

    @pl.when(me != n - 1)
    def _():
        sent = ext.at[pl.ds(0, back)]
        pltpu.make_async_copy(sent, sent, halo_send_next).wait()

    sent = ext.at[pl.ds(0, block)]
    pltpu.make_async_copy(sent, sent, halo_send_prev).wait()
    pltpu.make_async_copy(arrived, arrived, data_send).wait()
    pltpu.make_async_copy(others, others, power_send).wait()
    pltpu.make_async_copy(columns, columns, power_send_mid).wait()


def finish(rows, turn_ref, gain_ref, spectra_ref, out_ref):
    for q in range(spectra_ref.shape[1] // 2):
        for part in range(2):
            turned = lax.dot_general(
                turn_ref[...],
                spectra_ref[:, 2 * q + part].reshape(-1, LANES),
                (((1,), (1,)), ((), ())),
                preferred_element_type=jnp.float32,
            )
            for s in range(4):
                gain = gain_ref[4 * q + s : 4 * q + s + 1, :1]
                scaled = turned[s * rows : (s + 1) * rows, :] * gain
                out_ref[4 * q + s, part] = jnp.clip(scaled, -1.0, 1.0).astype(jnp.bfloat16)


def solution(mesh):
    n = mesh.shape["tm"]
    side = math.isqrt(n // 2)

    def on_device(samples, filter_taps):
        streams, length = samples.shape
        taps, fft_len = filter_taps.shape
        frames = length // fft_len
        rows = fft_len // LANES
        half = rows
        block = frames // 2
        back = taps - 1 - block
        first, twiddle, second, turn = constants(streams, rows, half)
        first = jnp.asarray(first, jnp.bfloat16)
        second = jnp.asarray(second, jnp.bfloat16)
        eye = jnp.asarray(turn, jnp.bfloat16)
        dims = (n, side, frames, taps, fft_len, streams, rows, half)
        tiles = streams // 4
        per = fft_len // 2 // n

        def body(*refs):
            kernel(dims, *refs)

        anywhere = pl.BlockSpec(memory_space=pltpu.HBM)
        dma = pltpu.SemaphoreType.DMA
        spectra, gain = pl.pallas_call(
            body,
            out_shape=(
                jax.ShapeDtypeStruct((2 * n, 2 * tiles, block, LANES), jnp.bfloat16),
                jax.ShapeDtypeStruct((streams, LANES), jnp.float32),
            ),
            in_specs=[anywhere] * 5,
            out_specs=(anywhere, pl.BlockSpec(memory_space=pltpu.VMEM)),
            scratch_shapes=[
                pltpu.VMEM((back + frames + block, streams, fft_len), jnp.bfloat16),
                pltpu.VMEM((taps, fft_len), jnp.bfloat16),
                pltpu.VMEM((rows, taps, streams, LANES), jnp.float32),
                pltpu.VMEM(first.shape, jnp.bfloat16),
                pltpu.VMEM(twiddle.shape, jnp.float32),
                pltpu.VMEM(second.shape, jnp.bfloat16),
                pltpu.VMEM((block, rows * streams, LANES), jnp.bfloat16),
                pltpu.VMEM((2, first.shape[0], 2 * LANES), jnp.float32),
                pltpu.VMEM((2 * tiles, block * PITCH, LANES), jnp.float32),
                pltpu.VMEM((2, n, 2 * tiles, block, LANES), jnp.bfloat16),
                pltpu.VMEM((tiles, block, LANES), jnp.float32),
                pltpu.VMEM((1, LANES), jnp.float32),
                pltpu.VMEM((2 * side, 1, LANES), jnp.float32),
                pltpu.VMEM((1, LANES), jnp.float32),
                pltpu.VMEM((side, 1, LANES), jnp.float32),
                dma((5 + frames,)),
                dma,
                dma,
                dma,
                dma,
                dma,
                dma,
                dma,
                dma,
                dma,
                dma,
                pltpu.SemaphoreType.REGULAR,
                pltpu.SemaphoreType.REGULAR,
                pltpu.SemaphoreType.REGULAR,
                pltpu.SemaphoreType.REGULAR,
                pltpu.SemaphoreType.REGULAR,
            ],
            compiler_params=pltpu.CompilerParams(
                collective_id=1, has_side_effects=True, vmem_limit_bytes=63 * 1024 * 1024
            ),
        )(samples, filter_taps, first, jnp.asarray(twiddle), second)

        cols = 1024

        def by_half(i):
            return (lax.rem(lax.axis_index("tm"), 2), 0, 0)

        return pl.pallas_call(
            functools.partial(finish, rows // 2),
            grid=(frames * n // cols,),
            out_shape=jax.ShapeDtypeStruct((streams, 2, per, frames * n), jnp.bfloat16),
            in_specs=[
                pl.BlockSpec((None, LANES, LANES), by_half),
                pl.BlockSpec((streams, LANES), lambda i: (0, 0)),
                pl.BlockSpec((cols // block, 2 * tiles, block, LANES), lambda i: (i, 0, 0, 0)),
            ],
            out_specs=pl.BlockSpec((streams, 2, per, cols), lambda i: (0, 0, 0, i)),
        )(eye, gain, spectra)

    return jax.shard_map(
        on_device,
        mesh=mesh,
        in_specs=(P("grp", "tm"), P()),
        out_specs=P("grp", None, "tm", None),
        check_vma=False,
    )
```
